128 devices in a mesh: dp: 8 (over x, core), crop: 4 (over y), tensor: 4 (over z).
Axes of the slice: x: 4, y: 4, z: 4, core: 2. Of those that a mesh axis runs over, the one named last changes fastest.
Arguments:
- hidden_a: bfloat16 [2048, 8192], P('crop', 'dp'), as said below
- hidden_b: bfloat16 [2048, 8192], P('crop', 'dp'), as said below
- weight: bfloat16 [8192, 8192], P('dp', 'tensor')
Outputs:
- weight_grad: float32 [8192, 8192], P(('dp', 'crop'), 'tensor')
Inputs may be any that keep to these rules, and one draw needn't show every extreme that they name: `hidden_a`: nonnegative entries. `hidden_b`: nonnegative entries.
All inputs are finite; a program needn't handle non-finite values.
Results may differ from the reference program's by a relative error of at most 0.0015.
Values may be sent and summed in bfloat16 or wider, within the bound.
A program may use at most 128 MiB of HBM per device.

```python
import jax
import jax.numpy as jnp
from jax import lax

H = 8192
F = 8192
B = 2048


def rising_scale(low, high, count):
    position = jnp.arange(count, dtype=jnp.float32) / jnp.float32(max(count - 1, 1))
    level = jnp.exp(jnp.log(jnp.float32(low)) + position * (jnp.log(jnp.float32(high)) - jnp.log(jnp.float32(low))))
    return level / jnp.sqrt(jnp.mean(level * level))


def hidden_pair(key):
    shared = jnp.clip(jax.random.normal(jax.random.fold_in(key, 21), (B, H), jnp.float32), -6.0, 6.0)
    left_noise = jnp.clip(jax.random.normal(jax.random.fold_in(key, 22), (B, H), jnp.float32), -6.0, 6.0)
    right_noise = jnp.clip(jax.random.normal(jax.random.fold_in(key, 23), (B, H), jnp.float32), -6.0, 6.0)
    row_scale = rising_scale(0.5, 2.5, B)[:, None]
    left = jnp.maximum(shared + 0.6 * left_noise, 0.0) * row_scale
    right = jnp.maximum(shared + 0.6 * right_noise, 0.0) * row_scale
    return (left, right)


def draw_hidden_a(key, part):
    return hidden_pair(key)[0].astype(jnp.bfloat16)


def draw_hidden_b(key, part):
    return hidden_pair(key)[1].astype(jnp.bfloat16)


def draw_weight(key, part):
    base_key = jax.random.fold_in(key, 11)
    band_key = jax.random.fold_in(key, 12)
    level_key = jax.random.fold_in(key, 13)
    base = jnp.clip(jax.random.normal(base_key, (H, F), jnp.float32), -6.0, 6.0) / jnp.sqrt(jnp.float32(H))
    upper = jax.random.bernoulli(band_key, 0.5, (F,))
    level = jax.random.uniform(level_key, (F,), jnp.float32)
    low_scale = jnp.exp(jnp.log(0.4) + level * (jnp.log(0.9) - jnp.log(0.4)))
    high_scale = jnp.exp(jnp.log(2.4) + level * (jnp.log(3.6) - jnp.log(2.4)))
    column_scale = jnp.where(upper, high_scale, low_scale)
    return (base * column_scale[None, :]).astype(jnp.bfloat16)


def setup_inputs(seed: int = 0) -> dict:
    key_of = jax.random.split(jax.random.key(seed), 4)
    hidden_a = draw_hidden_a(jax.random.fold_in(key_of[3], 71), 0)
    hidden_b = draw_hidden_b(jax.random.fold_in(key_of[3], 71), 0)
    weight = draw_weight(jax.random.fold_in(key_of[3], 71), 0)
    return dict(hidden_a=hidden_a, hidden_b=hidden_b, weight=weight)


epsilon = 0.0001

def reference(hidden_a, hidden_b, weight):
    total_rows = hidden_a.shape[0]
    left_proj = jnp.dot(hidden_a, weight, preferred_element_type=jnp.float32).astype(jnp.bfloat16)
    right_proj = jnp.dot(hidden_b, weight, preferred_element_type=jnp.float32).astype(jnp.bfloat16)
    stacked = jnp.stack([left_proj, right_proj]).astype(jnp.float32)
    col_means = lax.optimization_barrier(jnp.mean(stacked, axis=1))
    centered = stacked - col_means[:, None, :]
    spread = lax.optimization_barrier(jnp.sum(centered * centered, axis=1))
    deviation = jnp.sqrt(spread / (total_rows - 1.0) + epsilon)
    rounded = centered.astype(jnp.bfloat16)
    products = []
    for branch in range(2):
        gram_full = lax.dot_general(rounded[branch], rounded[branch], (((1,), (1,)), ((), ())), preferred_element_type=jnp.float32)
        products.append(jnp.dot(gram_full.astype(jnp.bfloat16), rounded[branch], preferred_element_type=jnp.float32))
    products = jnp.stack(products)
    hinge_rate = jnp.where(deviation < 1.0, 25.0 / ((total_rows - 1.0) * deviation), 0.0)[:, None, :]
    differ = stacked[0] - stacked[1]
    pull_term = jnp.stack([differ, -differ]) * (50.0 / total_rows)
    cov_scale = 4.0 / (total_rows - 1.0) ** 2
    row_grads = pull_term - hinge_rate * centered + cov_scale * (products - centered * spread[:, None, :])
    row_grads = row_grads.astype(jnp.bfloat16)
    across = (((0,), (0,)), ((), ()))
    left_term = lax.dot_general(hidden_a, row_grads[0], across, preferred_element_type=jnp.float32)
    right_term = lax.dot_general(hidden_b, row_grads[1], across, preferred_element_type=jnp.float32)
    return left_term + right_term
```

```python
import functools

import jax
import jax.numpy as jnp
from jax import lax
from jax.experimental import pallas as pl
from jax.experimental.pallas import tpu as pltpu
from jax.sharding import PartitionSpec as P

MESH = pl.DeviceIdType.MESH
BF, F32 = jnp.bfloat16, jnp.float32
NSEM = 144
EPS = 0.0001
FULL = slice(None)


def mm(a, b, dims=(((1,), (0,)), ((), ()))):
    return lax.dot_general(a, b, dims, preferred_element_type=F32)


def kernel(ha, hb, w, out, hc, wb, acc, s_far, s_raw, s_acc, r_far, r_raw, r_acc, zb, cb, hall,
           ht, mx, my, mu, dd, dsum, gf, gb, gr, gp, lt, orecv, send, recv, lsem):
    dp = lax.axis_index("dp")
    y = lax.axis_index("crop")
    t = lax.axis_index("tensor")
    x, c = lax.div(dp, 2), lax.rem(dp, 2)
    rows = 2048
    alpha = 50.0 / rows
    cov = 4.0 / (rows - 1.0) ** 2
    sign = jnp.where(c == 0, 1.0, -1.0).astype(F32)

    def turn(v, k):
        return lax.rem(v + k + 4, 4)

    def at_x(k):
        return (2 * turn(x, k) + c, y, t)

    def at_y(k):
        return (dp, turn(y, k), t)

    def at_t(k):
        return (dp, y, turn(t, k))

    partner = (2 * x + 1 - c, y, t)
    count = [0]
    started = []

    def remote(src, dst, dev, index=None):
        if index is None:
            index = count[0]
            count[0] += 1
        return pltpu.make_async_remote_copy(
            src_ref=src, dst_ref=dst, send_sem=send.at[index], recv_sem=recv.at[index],
            device_id=dev, device_id_type=MESH)

    def go(src, dst, dev):
        copy = remote(src, dst, dev)
        copy.start()
        started.append(copy)
        return copy

    def load(src, dst, i):
        return pltpu.make_async_copy(src, dst, lsem.at[i])

    load_w = [load(w.at[:, pl.ds(512 * j, 512)], wb.at[c, :, pl.ds(512 * j, 512)], j) for j in range(4)]
    load_h = load(ha, hc.at[c], 4)
    own = [load(h.at[:, pl.ds(256 * y, 256)], hall.at[v, c, y], 5 + v) for v, h in enumerate((ha, hb))]

    @pl.when(c == 0)
    def _():
        load(ha, hc.at[c], 4).start()

    @pl.when(c == 1)
    def _():
        load(hb, hc.at[c], 4).start()

    for copy in load_w + own:
        copy.start()

    barrier = pltpu.get_barrier_semaphore()
    peers = [partner] + [f(k) for f in (at_x, at_y, at_t) for k in (1, 2, 3)]
    for peer in peers:
        pl.semaphore_signal(barrier, inc=1, device_id=peer, device_id_type=MESH)
    pl.semaphore_wait(barrier, len(peers))

    h_index = count[0]
    count[0] += 1

    @pl.when(c == 0)
    def _():
        remote(hb, hc.at[c], partner, h_index).start()

    @pl.when(c == 1)
    def _():
        remote(ha, hc.at[c], partner, h_index).start()

    swap_h = remote(ha, hc.at[c], partner, h_index)
    started.append(swap_h)
    swap_w = [go(w.at[:, pl.ds(512 * j, 512)], wb.at[c, :, pl.ds(512 * j, 512)], partner) for j in range(4)]

    deal = []
    for k in (1, 3, 2):
        for v, h in enumerate((ha, hb)):
            deal.append((k, v, go(h.at[:, pl.ds(256 * turn(y, k), 256)], hall.at[v, c, y], at_y(k))))

    load_h.wait()
    swap_h.wait_recv()

    def way(j):
        return 1 if j % 2 == 0 else -1

    far, raw, summed = {}, {}, {}

    def relay(j):
        d = way(j)
        far[j].wait_recv()
        s_acc[j] = (acc[j, pl.ds(128 * turn(x, d), 128), :] + r_far[j].astype(F32)).astype(BF)
        summed[j] = go(s_acc.at[j], r_acc.at[j], at_x(d))

    for j in range(4):
        load_w[j].wait()
        swap_w[j].wait_recv()

        def half(n, _):
            cols = pl.ds(pl.multiple_of(512 * j + 256 * n, 256), 256)
            acc[j, :, pl.ds(pl.multiple_of(256 * n, 256), 256)] = (
                mm(hc[0], wb[0, :, cols]) + mm(hc[1], wb[1, :, cols]))
            return 0

        lax.fori_loop(0, 2, half, 0)
        d = way(j)
        s_far[j] = acc[j, pl.ds(128 * turn(x, 2), 128), :].astype(BF)
        s_raw[j] = acc[j, pl.ds(128 * turn(x, -d), 128), :].astype(BF)
        far[j] = go(s_far.at[j], r_far.at[j], at_x(d))
        raw[j] = go(s_raw.at[j], r_raw.at[j], at_x(-d))
        if j > 0:
            relay(j - 1)
    relay(3)

    block = 4 * y + x
    for j in range(4):
        raw[j].wait_recv()
        summed[j].wait_recv()
        cols = slice(512 * j, 512 * j + 512)
        z = (acc[j, pl.ds(128 * x, 128), :] + r_raw[j].astype(F32) + r_acc[j].astype(F32)).astype(BF)
        zb[block, :, cols] = z
        mx[x, :, cols] = jnp.sum(z.astype(F32), axis=0, keepdims=True)

    cols_of = (pl.ds(0, 1024), pl.ds(1024, 1024))

    class Ring:
        def __init__(self, axis, colour, offset):
            self.axis, self.colour, self.offset = axis, colour, offset
            self.to = at_x if axis == 0 else at_y
            self.right = go(self.piece(0), self.piece(0), self.to(1))
            self.left = go(self.piece(0), self.piece(0), self.to(-1))

        def index(self, k):
            if self.axis == 0:
                return 4 * turn(y, self.offset) + turn(x, k)
            return 4 * turn(y, k) + turn(x, self.offset)

        def piece(self, k, part=pl.ds(0, 128)):
            return zb.at[self.index(k), part, cols_of[self.colour]]

        def take(self):
            low, high = pl.ds(0, 64), pl.ds(64, 64)
            self.right.wait_recv()
            self.on_right = go(self.piece(-1, low), self.piece(-1, low), self.to(1))
            self.left.wait_recv()
            self.on_left = go(self.piece(1, high), self.piece(1, high), self.to(-1))

        def end(self):
            self.on_right.wait_recv()
            self.on_left.wait_recv()

    x_first = Ring(0, 0, 0)
    y_first = Ring(1, 1, 0)
    x_rings = {0: Ring(0, 1, 0)}
    y_rings = {0: Ring(1, 0, 0)}

    hops = [go(mx.at[x], mx.at[x], at_x(k)) for k in (1, 3, 2)]
    for hop in hops:
        hop.wait_recv()
    my[y] = mx[0] + mx[1] + mx[2] + mx[3]
    hops = [go(my.at[y], my.at[y], at_y(k)) for k in (1, 3, 2)]
    for hop in hops:
        hop.wait_recv()
    mu[...] = (my[0] + my[1] + my[2] + my[3]) * (1.0 / rows)
    dd[...] = jnp.zeros_like(dd)

    def center(index, colour):
        cols = slice(1024 * colour, 1024 * colour + 1024)
        cent = zb[index, :, cols].astype(F32) - mu[:, cols]
        dd[:, cols] += jnp.sum(cent * cent, axis=0, keepdims=True)
        cb[index, :, cols] = cent.astype(BF)

    def center_ring(ring, ks):
        for k in ks:
            center(ring.index(k), ring.colour)

    center(block, 0)
    center(block, 1)

    for v in range(2):
        own[v].wait()
        deal.append((0, v, None))
    handed = []
    for k, v, copy in sorted(deal, key=lambda item: (item[0] != 0)):
        if copy is not None:
            copy.wait_recv()
        slot = hall.at[v, c, turn(y, -k)]
        handed.append(go(slot, slot, partner))

    x_first.take()
    for k in (-1, 1):
        y_rings[k] = Ring(1, 0, k)
    y_first.take()
    for k in (-1, 1):
        x_rings[k] = Ring(0, 1, k)
    center_ring(x_first, (-1, 1))
    center_ring(y_first, (-1, 1))
    x_rings[0].take()
    y_rings[0].take()
    x_first.end()
    y_rings[2] = Ring(1, 0, 2)
    y_first.end()
    x_rings[2] = Ring(0, 1, 2)
    center_ring(x_first, (2,))
    center_ring(y_first, (2,))
    center_ring(x_rings[0], (-1, 1))
    center_ring(y_rings[0], (-1, 1))

    for copy in handed:
        copy.wait_recv()

    def flip(i, _):
        v, r = lax.div(i, 16), lax.rem(i, 16)
        k, yy = lax.div(r, 8), lax.div(lax.rem(r, 8), 2)
        part = lax.rem(r, 2)
        where = pl.multiple_of(512 * yy + 256 * part, 256)
        tile = hall[v, k, yy, pl.ds(pl.multiple_of(256 * part, 256), 256), :]
        ht[v, pl.ds(pl.multiple_of(256 * k, 256), 256), pl.ds(where, 256)] = tile.T
        return 0

    before = 0
    for k in (-1, 1, 2):
        x_rings[k].take()
        y_rings[k].take()
        before_ring = {-1: 0, 1: -1, 2: 1}[k]
        x_rings[before_ring].end()
        y_rings[before_ring].end()
        center_ring(x_rings[before_ring], (2,))
        center_ring(y_rings[before_ring], (2,))
        center_ring(x_rings[k], (-1, 1))
        center_ring(y_rings[k], (-1, 1))
        if k == -1:
            lax.fori_loop(0, 32, flip, 0)

            def add_up(i, _):
                part = pl.ds(pl.multiple_of(128 * i, 128), 128)
                diff = ht[0, part, :].astype(F32) - ht[1, part, :].astype(F32)
                dsum[part, :] = jnp.sum(diff, axis=1, keepdims=True)
                return 0

            lax.fori_loop(0, 4, add_up, 0)
    x_rings[2].end()
    y_rings[2].end()
    center_ring(x_rings[2], (2,))
    center_ring(y_rings[2], (2,))

    mine = cb[block]

    def pair(p, _):
        one = cb[lax.rem(block + 2 * p, 16)]
        two = cb[lax.rem(block + 2 * p + 1, 16)]
        res = mm(mine, jnp.concatenate([one, two], axis=0), (((1,), (1,)), ((), ())))
        at = pl.ds(pl.multiple_of(256 * p, 256), 256)
        gf[:, at] = res
        gb[:, at] = res.astype(BF)
        return 0

    lax.fori_loop(0, 4, pair, 0)
    last = mm(mine, cb[lax.rem(block + 8, 16)], (((1,), (1,)), ((), ())))
    gf[:, 1024:] = last
    gb[:, 1024:] = last.astype(BF)

    def strip(v):
        return pl.ds(pl.multiple_of(32 * v, 32), 32)

    hops = [go(gb.at[strip(turn(t, k)), :], gr.at[t], at_t(k)) for k in (1, 3, 2)]
    for hop in hops:
        hop.wait_recv()
    total = gf[strip(t), :]
    for k in (1, 2, 3):
        total = total + gr[turn(t, k)].astype(F32)
    gp[y, x, strip(t), :] = total.astype(BF)

    def part_of(n, i):
        return pl.ds(n * i, n)

    class Turn:
        def __init__(self, axis, colour, depth):
            self.axis = axis
            self.cols = pl.ds(384 * colour, 384)
            self.done = depth
            self.to = (at_x, at_y, at_t)[axis]
            self.right = go(self.piece(0, None), self.piece(0, None), self.to(1))
            self.left = go(self.piece(0, None), self.piece(0, None), self.to(-1))

        def piece(self, k, half):
            spots = [x, y, t]
            spots[self.axis] = turn(spots[self.axis], k)
            px, py, pt = spots
            ix = pl.ds(0, 4) if 0 in self.done else px
            iy = pl.ds(0, 4) if 1 in self.done else py
            it = pl.ds(0, 128) if 2 in self.done else strip(pt)
            if half is not None:
                if 1 in self.done:
                    iy = pl.ds(2 * half, 2)
                elif 0 in self.done:
                    ix = pl.ds(2 * half, 2)
                elif 2 in self.done:
                    it = pl.ds(64 * half, 64)
                else:
                    it = pl.ds(pl.multiple_of(32 * pt + 16 * half, 16), 16)
            return gp.at[iy, ix, it, self.cols]

        def take(self):
            self.right.wait_recv()
            self.on_right = go(self.piece(-1, 0), self.piece(-1, 0), self.to(1))
            self.left.wait_recv()
            self.on_left = go(self.piece(1, 1), self.piece(1, 1), self.to(-1))

        def end(self):
            self.on_right.wait_recv()
            self.on_left.wait_recv()

    orders = ((2, 1, 0), (0, 2, 1), (1, 0, 2))

    spread = dd[...]
    dev = jnp.sqrt(spread * (1.0 / (rows - 1.0)) + EPS)
    rate = jnp.where(dev < 1.0, 25.0 / ((rows - 1.0) * dev), 0.0) + cov * spread
    dd[...] = rate

    def plain(n, _):
        j, p = lax.div(n, 2), lax.rem(n, 2)
        cols = pl.ds(pl.multiple_of(256 * n, 256), 256)
        at = pl.ds(pl.multiple_of(256 * p, 256), 256)
        right = cb[:, :, cols].reshape(2048, 256)
        acc[j, :, at] = (sign * alpha) * dsum[...] * mu[:, cols] - mm(ht[c], right) * dd[:, cols]
        return 0

    cuts = (0, 2, 4, 8)
    for phase in range(3):
        turns = [Turn(order[phase], colour, order[:phase]) for colour, order in enumerate(orders)]
        lax.fori_loop(cuts[phase], cuts[phase + 1], plain, 0)
        for one in turns:
            one.take()
        for one in turns:
            one.end()

    for copy in started:
        copy.wait_send()
    started.clear()

    def spread_panel(b, _):
        by, bx = lax.div(b, 4), lax.rem(b, 4)
        here = pl.ds(pl.multiple_of(128 * b, 128), 128)
        for j in range(9):
            other = lax.rem(b + j, 16)
            tile = gp[by, bx, :, 128 * j:128 * j + 128]
            zb[b, :, pl.ds(pl.multiple_of(128 * other, 128), 128)] = tile
            if 0 < j < 8:
                zb[other, :, here] = tile.T
        return 0

    lax.fori_loop(0, 16, spread_panel, 0)

    def factor(n, _):
        cols = pl.ds(pl.multiple_of(256 * n, 256), 256)
        res = mm(ht[c], zb[:, :, cols].reshape(2048, 256))
        diff = ht[0, :, cols].astype(F32) - ht[1, :, cols].astype(F32)
        lt[:, cols] = (cov * res + (sign * alpha) * diff).astype(BF)
        return 0

    lax.fori_loop(0, 8, factor, 0)

    theirs = pl.ds(pl.multiple_of(256 * (1 - c), 256), 256)
    ours = pl.ds(pl.multiple_of(256 * c, 256), 256)

    def finish(which, j):
        def step(p, _):
            cols = pl.ds(pl.multiple_of(512 * j + 256 * p, 256), 256)
            at = pl.ds(pl.multiple_of(256 * p, 256), 256)
            acc[j, which, at] += mm(lt[which, :], cb[:, :, cols].reshape(2048, 256))
            return 0

        lax.fori_loop(0, 2, step, 0)

    give = []
    for j in range(4):
        finish(theirs, j)
        give.append(go(acc.at[j, theirs, :], orecv.at[j], partner))
    stores = []
    for j in range(4):
        finish(ours, j)
        give[j].wait_recv()
        orecv[j] += acc[j, ours, :]
        stores.append(load(orecv.at[j], out.at[:, pl.ds(512 * j, 512)], 7 + j))
        stores[j].start()
    for copy in started:
        copy.wait_send()
    for copy in stores:
        copy.wait()


def body(hidden_a, hidden_b, weight):
    anywhere = pl.BlockSpec(memory_space=pl.ANY)
    vm = pltpu.VMEM
    return pl.pallas_call(
        kernel,
        out_shape=jax.ShapeDtypeStruct((256, 2048), F32),
        in_specs=[anywhere] * 3,
        out_specs=anywhere,
        scratch_shapes=[
            vm((2, 512, 1024), BF), vm((2, 1024, 2048), BF), vm((4, 512, 512), F32),
            vm((4, 128, 512), BF), vm((4, 128, 512), BF), vm((4, 128, 512), BF),
            vm((4, 128, 512), BF), vm((4, 128, 512), BF), vm((4, 128, 512), BF),
            vm((16, 128, 2048), BF), vm((16, 128, 2048), BF), vm((2, 2, 4, 512, 256), BF),
            vm((2, 512, 2048), BF), vm((4, 1, 2048), F32), vm((4, 1, 2048), F32),
            vm((1, 2048), F32), vm((1, 2048), F32), vm((512, 1), F32),
            vm((128, 1152), F32), vm((128, 1152), BF), vm((4, 32, 1152), BF),
            vm((4, 4, 128, 1152), BF), vm((512, 2048), BF), vm((4, 256, 512), F32),
            pltpu.SemaphoreType.DMA((NSEM,)), pltpu.SemaphoreType.DMA((NSEM,)),
            pltpu.SemaphoreType.DMA((12,)),
        ],
        compiler_params=pltpu.CompilerParams(
            collective_id=0, has_side_effects=True, vmem_limit_bytes=67000000),
        name="vicreg_grad",
    )(hidden_a, hidden_b, weight)


def solution(mesh):
    placed = (P("crop", "dp"), P("crop", "dp"), P("dp", "tensor"))
    return jax.shard_map(
        body, mesh=mesh, in_specs=placed, out_specs=P(("dp", "crop"), "tensor"), check_vma=False
    )
```

```python
import functools

import jax
import jax.numpy as jnp
from jax import lax
from jax.experimental import pallas as pl
from jax.experimental.pallas import tpu as pltpu
from jax.sharding import PartitionSpec as P

MESH = pl.DeviceIdType.MESH
BF, F32 = jnp.bfloat16, jnp.float32
NSEM = 208
EPS = 0.0001
FULL = slice(None)


def mm(a, b, dims=(((1,), (0,)), ((), ()))):
    return lax.dot_general(a, b, dims, preferred_element_type=F32)


def kernel(ha, hb, w, out, hc, wb, acc, s_far, s_raw, s_acc, r_far, r_raw, r_acc, zb, cb, hall,
           ht, mx, my, mu, dd, dsum, gf, gb, gr, gp, lt, orecv, send, recv, lsem):
    dp = lax.axis_index("dp")
    y = lax.axis_index("crop")
    t = lax.axis_index("tensor")
    x, c = lax.div(dp, 2), lax.rem(dp, 2)
    rows = 2048
    alpha = 50.0 / rows
    cov = 4.0 / (rows - 1.0) ** 2
    sign = jnp.where(c == 0, 1.0, -1.0).astype(F32)

    def turn(v, k):
        return lax.rem(v + k + 4, 4)

    def at_x(k):
        return (2 * turn(x, k) + c, y, t)

    def at_y(k):
        return (dp, turn(y, k), t)

    def at_t(k):
        return (dp, y, turn(t, k))

    partner = (2 * x + 1 - c, y, t)
    count = [0]
    started = []

    def remote(src, dst, dev, index=None):
        if index is None:
            index = count[0]
            count[0] += 1
        return pltpu.make_async_remote_copy(
            src_ref=src, dst_ref=dst, send_sem=send.at[index], recv_sem=recv.at[index],
            device_id=dev, device_id_type=MESH)

    def go(src, dst, dev):
        copy = remote(src, dst, dev)
        copy.start()
        started.append(copy)
        return copy

    def load(src, dst, i):
        return pltpu.make_async_copy(src, dst, lsem.at[i])

    load_w = [load(w.at[:, pl.ds(512 * j, 512)], wb.at[c, :, pl.ds(512 * j, 512)], j) for j in range(4)]
    load_h = load(ha, hc.at[c], 4)
    own = [load(h.at[:, pl.ds(256 * y, 256)], hall.at[v, c, y], 5 + v) for v, h in enumerate((ha, hb))]

    @pl.when(c == 0)
    def _():
        load(ha, hc.at[c], 4).start()

    @pl.when(c == 1)
    def _():
        load(hb, hc.at[c], 4).start()

    for copy in load_w + own:
        copy.start()

    barrier = pltpu.get_barrier_semaphore()
    peers = [partner] + [f(k) for f in (at_x, at_y, at_t) for k in (1, 2, 3)]
    for peer in peers:
        pl.semaphore_signal(barrier, inc=1, device_id=peer, device_id_type=MESH)
    pl.semaphore_wait(barrier, len(peers))

    h_index = count[0]
    count[0] += 1

    @pl.when(c == 0)
    def _():
        remote(hb, hc.at[c], partner, h_index).start()

    @pl.when(c == 1)
    def _():
        remote(ha, hc.at[c], partner, h_index).start()

    swap_h = remote(ha, hc.at[c], partner, h_index)
    started.append(swap_h)
    swap_w = [go(w.at[:, pl.ds(512 * j, 512)], wb.at[c, :, pl.ds(512 * j, 512)], partner) for j in range(4)]

    def quarter(v):
        return pl.ds(pl.multiple_of(128 * v, 128), 128)

    deal = []
    for k in (1, 3, 2):
        for v, h in enumerate((ha, hb)):
            deal.append((k, v, go(h.at[quarter(t), pl.ds(256 * turn(y, k), 256)], hall.at[v, c, y, quarter(t)], at_y(k))))

    load_h.wait()
    swap_h.wait_recv()

    def way(j):
        return 1 if j % 2 == 0 else -1

    far, raw, summed = {}, {}, {}

    def relay(j):
        d = way(j)
        far[j].wait_recv()
        s_acc[j] = (acc[j, pl.ds(128 * turn(x, d), 128), :] + r_far[j].astype(F32)).astype(BF)
        summed[j] = go(s_acc.at[j], r_acc.at[j], at_x(d))

    for j in range(4):
        load_w[j].wait()
        swap_w[j].wait_recv()

        def half(n, _):
            cols = pl.ds(pl.multiple_of(512 * j + 256 * n, 256), 256)
            acc[j, :, pl.ds(pl.multiple_of(256 * n, 256), 256)] = (
                mm(hc[0], wb[0, :, cols]) + mm(hc[1], wb[1, :, cols]))
            return 0

        lax.fori_loop(0, 2, half, 0)
        d = way(j)
        s_far[j] = acc[j, pl.ds(128 * turn(x, 2), 128), :].astype(BF)
        s_raw[j] = acc[j, pl.ds(128 * turn(x, -d), 128), :].astype(BF)
        far[j] = go(s_far.at[j], r_far.at[j], at_x(d))
        raw[j] = go(s_raw.at[j], r_raw.at[j], at_x(-d))
        if j > 0:
            relay(j - 1)
    relay(3)

    block = 4 * y + x
    for j in range(4):
        raw[j].wait_recv()
        summed[j].wait_recv()
        cols = slice(512 * j, 512 * j + 512)
        z = (acc[j, pl.ds(128 * x, 128), :] + r_raw[j].astype(F32) + r_acc[j].astype(F32)).astype(BF)
        zb[block, :, cols] = z
        mx[x, :, cols] = jnp.sum(z.astype(F32), axis=0, keepdims=True)

    cols_of = (pl.ds(0, 1024), pl.ds(1024, 1024))

    class Ring:
        def __init__(self, axis, colour, offset):
            self.axis, self.colour, self.offset = axis, colour, offset
            self.to = at_x if axis == 0 else at_y
            self.right = go(self.piece(0), self.piece(0), self.to(1))
            self.left = go(self.piece(0), self.piece(0), self.to(-1))

        def index(self, k):
            if self.axis == 0:
                return 4 * turn(y, self.offset) + turn(x, k)
            return 4 * turn(y, k) + turn(x, self.offset)

        def piece(self, k, part=pl.ds(0, 128)):
            return zb.at[self.index(k), part, cols_of[self.colour]]

        def take(self):
            low, high = pl.ds(0, 64), pl.ds(64, 64)
            self.right.wait_recv()
            self.on_right = go(self.piece(-1, low), self.piece(-1, low), self.to(1))
            self.left.wait_recv()
            self.on_left = go(self.piece(1, high), self.piece(1, high), self.to(-1))

        def end(self):
            self.on_right.wait_recv()
            self.on_left.wait_recv()

    x_first = Ring(0, 0, 0)
    y_first = Ring(1, 1, 0)
    x_rings = {0: Ring(0, 1, 0)}
    y_rings = {0: Ring(1, 0, 0)}

    hops = [go(mx.at[x], mx.at[x], at_x(k)) for k in (1, 3, 2)]
    for hop in hops:
        hop.wait_recv()
    my[y] = mx[0] + mx[1] + mx[2] + mx[3]
    hops = [go(my.at[y], my.at[y], at_y(k)) for k in (1, 3, 2)]
    for hop in hops:
        hop.wait_recv()
    mu[...] = (my[0] + my[1] + my[2] + my[3]) * (1.0 / rows)
    dd[...] = jnp.zeros_like(dd)

    def center(index, colour):
        cols = slice(1024 * colour, 1024 * colour + 1024)
        cent = zb[index, :, cols].astype(F32) - mu[:, cols]
        dd[:, cols] += jnp.sum(cent * cent, axis=0, keepdims=True)
        cb[index, :, cols] = cent.astype(BF)

    def center_ring(ring, ks):
        for k in ks:
            center(ring.index(k), ring.colour)

    center(block, 0)
    center(block, 1)

    class Rows:
        def __init__(self, k, v):
            self.slot = hall.at[v, c, turn(y, -k)]
            mine = self.slot.at[quarter(t)]
            self.right, self.left = go(mine, mine, at_t(1)), go(mine, mine, at_t(-1))

        def take(self):
            self.right.wait_recv()
            piece = self.slot.at[pl.ds(pl.multiple_of(128 * turn(t, -1), 128), 64)]
            self.on_right = go(piece, piece, at_t(1))
            self.left.wait_recv()
            piece = self.slot.at[pl.ds(pl.multiple_of(128 * turn(t, 1) + 64, 64), 64)]
            self.on_left = go(piece, piece, at_t(-1))

        def end(self):
            self.on_right.wait_recv()
            self.on_left.wait_recv()

    handed = []
    for v in range(2):
        own[v].wait()
        handed.append(go(hall.at[v, c, y], hall.at[v, c, y], partner))
    spans = []
    for k, v, copy in deal:
        copy.wait_recv()
        spans.append(Rows(k, v))

    x_first.take()
    for k in (-1, 1):
        y_rings[k] = Ring(1, 0, k)
    y_first.take()
    for k in (-1, 1):
        x_rings[k] = Ring(0, 1, k)
    center_ring(x_first, (-1, 1))
    center_ring(y_first, (-1, 1))
    for span in spans:
        span.take()
    x_rings[0].take()
    y_rings[0].take()
    x_first.end()
    y_rings[2] = Ring(1, 0, 2)
    y_first.end()
    x_rings[2] = Ring(0, 1, 2)
    center_ring(x_first, (2,))
    center_ring(y_first, (2,))
    center_ring(x_rings[0], (-1, 1))
    center_ring(y_rings[0], (-1, 1))

    for span in spans:
        span.end()
        handed.append(go(span.slot, span.slot, partner))

    def flip(i, _):
        v, r = lax.div(i, 16), lax.rem(i, 16)
        k, yy = lax.div(r, 8), lax.div(lax.rem(r, 8), 2)
        part = lax.rem(r, 2)
        where = pl.multiple_of(512 * yy + 256 * part, 256)
        tile = hall[v, k, yy, pl.ds(pl.multiple_of(256 * part, 256), 256), :]
        ht[v, pl.ds(pl.multiple_of(256 * k, 256), 256), pl.ds(where, 256)] = tile.T
        return 0

    for k in (-1, 1, 2):
        x_rings[k].take()
        y_rings[k].take()
        before_ring = {-1: 0, 1: -1, 2: 1}[k]
        x_rings[before_ring].end()
        y_rings[before_ring].end()
        center_ring(x_rings[before_ring], (2,))
        center_ring(y_rings[before_ring], (2,))
        center_ring(x_rings[k], (-1, 1))
        center_ring(y_rings[k], (-1, 1))
        if k == -1:
            for copy in handed:
                copy.wait_recv()
            lax.fori_loop(0, 32, flip, 0)

            def add_up(i, _):
                part = pl.ds(pl.multiple_of(128 * i, 128), 128)
                diff = ht[0, part, :].astype(F32) - ht[1, part, :].astype(F32)
                dsum[part, :] = jnp.sum(diff, axis=1, keepdims=True)
                return 0

            lax.fori_loop(0, 4, add_up, 0)
    x_rings[2].end()
    y_rings[2].end()
    center_ring(x_rings[2], (2,))
    center_ring(y_rings[2], (2,))

    mine = cb[block]

    def pair(p, _):
        one = cb[lax.rem(block + 2 * p, 16)]
        two = cb[lax.rem(block + 2 * p + 1, 16)]
        res = mm(mine, jnp.concatenate([one, two], axis=0), (((1,), (1,)), ((), ())))
        at = pl.ds(pl.multiple_of(256 * p, 256), 256)
        gf[:, at] = res
        gb[:, at] = res.astype(BF)
        return 0

    lax.fori_loop(0, 4, pair, 0)
    last = mm(mine, cb[lax.rem(block + 8, 16)], (((1,), (1,)), ((), ())))
    gf[:, 1024:] = last
    gb[:, 1024:] = last.astype(BF)

    def strip(v):
        return pl.ds(pl.multiple_of(32 * v, 32), 32)

    hops = [go(gb.at[strip(turn(t, k)), :], gr.at[t], at_t(k)) for k in (1, 3, 2)]
    for hop in hops:
        hop.wait_recv()
    total = gf[strip(t), :]
    for k in (1, 2, 3):
        total = total + gr[turn(t, k)].astype(F32)
    gp[y, x, strip(t), :] = total.astype(BF)

    class Turn:
        def __init__(self, axis, colour, done, fixed=None, offset=0):
            self.axis, self.done, self.fixed, self.offset = axis, done, fixed, offset
            self.cols = pl.ds(384 * colour, 384)
            self.to = (at_x, at_y, at_t)[axis]
            self.sent = [go(self.piece(0), self.piece(0), self.to(k)) for k in ((1, -1) if done else (1, -1, 2))]

        def piece(self, k, half=None):
            spots = [x, y, t]
            if self.fixed is not None:
                spots[self.fixed] = turn(spots[self.fixed], self.offset)
            spots[self.axis] = turn(spots[self.axis], k)
            ix, iy, it = spots[0], spots[1], strip(spots[2])
            if half is None:
                whole = {0: pl.ds(0, 4), 1: pl.ds(0, 4), 2: pl.ds(0, 128)}
            else:
                whole = {0: pl.ds(2 * half, 2), 1: pl.ds(2 * half, 2), 2: pl.ds(64 * half, 64)}
            ix = whole[0] if self.done == 0 + 1 else ix
            iy = whole[1] if self.done == 1 + 1 else iy
            it = whole[2] if self.done == 2 + 1 else it
            return gp.at[iy, ix, it, self.cols]

        def take(self):
            self.sent[0].wait_recv()
            self.on_right = go(self.piece(-1, 0), self.piece(-1, 0), self.to(1))
            self.sent[1].wait_recv()
            self.on_left = go(self.piece(1, 1), self.piece(1, 1), self.to(-1))

        def end(self):
            self.on_right.wait_recv()
            self.on_left.wait_recv()

    orders = ((2, 1, 0), (0, 2, 1), (1, 0, 2))

    spread = dd[...]
    dev = jnp.sqrt(spread * (1.0 / (rows - 1.0)) + EPS)
    rate = jnp.where(dev < 1.0, 25.0 / ((rows - 1.0) * dev), 0.0) + cov * spread
    dd[...] = rate

    def plain(n, _):
        j, p = lax.div(n, 2), lax.rem(n, 2)
        cols = pl.ds(pl.multiple_of(256 * n, 256), 256)
        at = pl.ds(pl.multiple_of(256 * p, 256), 256)
        right = cb[:, :, cols].reshape(2048, 256)
        acc[j, :, at] = (sign * alpha) * dsum[...] * mu[:, cols] - mm(ht[c], right) * dd[:, cols]
        return 0

    firsts = [Turn(a, i, 0) for i, (a, b, d) in enumerate(orders)]
    lax.fori_loop(0, 2, plain, 0)
    for first in firsts:
        for copy in first.sent:
            copy.wait_recv()
    seconds = [Turn(b, i, a + 1) for i, (a, b, d) in enumerate(orders)]

    def third(offset):
        return [Turn(d, i, a + 1, b, offset) for i, (a, b, d) in enumerate(orders)]

    def take(turns):
        for one in turns:
            one.take()

    def end(turns):
        for one in turns:
            one.end()

    thirds = {0: third(0)}
    lax.fori_loop(2, 4, plain, 0)
    take(seconds)
    thirds[-1] = third(-1)
    thirds[1] = third(1)
    take(thirds[0])
    lax.fori_loop(4, 6, plain, 0)
    end(seconds)
    thirds[2] = third(2)
    lax.fori_loop(6, 7, plain, 0)
    take(thirds[-1])
    end(thirds[0])
    take(thirds[1])
    lax.fori_loop(7, 8, plain, 0)
    take(thirds[2])
    for offset in (-1, 1, 2):
        end(thirds[offset])

    for copy in started:
        copy.wait_send()
    started.clear()

    def spread_panel(b, _):
        by, bx = lax.div(b, 4), lax.rem(b, 4)
        here = pl.ds(pl.multiple_of(128 * b, 128), 128)
        for j in range(9):
            other = lax.rem(b + j, 16)
            tile = gp[by, bx, :, 128 * j:128 * j + 128]
            zb[b, :, pl.ds(pl.multiple_of(128 * other, 128), 128)] = tile
            if 0 < j < 8:
                zb[other, :, here] = tile.T
        return 0

    lax.fori_loop(0, 16, spread_panel, 0)

    def factor(n, _):
        cols = pl.ds(pl.multiple_of(256 * n, 256), 256)
        res = mm(ht[c], zb[:, :, cols].reshape(2048, 256))
        diff = ht[0, :, cols].astype(F32) - ht[1, :, cols].astype(F32)
        lt[:, cols] = (cov * res + (sign * alpha) * diff).astype(BF)
        return 0

    lax.fori_loop(0, 8, factor, 0)

    theirs = pl.ds(pl.multiple_of(256 * (1 - c), 256), 256)
    ours = pl.ds(pl.multiple_of(256 * c, 256), 256)

    def finish(which, j):
        def step(p, _):
            cols = pl.ds(pl.multiple_of(512 * j + 256 * p, 256), 256)
            at = pl.ds(pl.multiple_of(256 * p, 256), 256)
            acc[j, which, at] += mm(lt[which, :], cb[:, :, cols].reshape(2048, 256))
            return 0

        lax.fori_loop(0, 2, step, 0)

    give = []
    for j in range(4):
        finish(theirs, j)
        give.append(go(acc.at[j, theirs, :], orecv.at[j], partner))
    stores = []
    for j in range(4):
        finish(ours, j)
        give[j].wait_recv()
        orecv[j] += acc[j, ours, :]
        stores.append(load(orecv.at[j], out.at[:, pl.ds(512 * j, 512)], 7 + j))
        stores[j].start()
    for copy in started:
        copy.wait_send()
    for copy in stores:
        copy.wait()


def body(hidden_a, hidden_b, weight):
    anywhere = pl.BlockSpec(memory_space=pl.ANY)
    vm = pltpu.VMEM
    return pl.pallas_call(
        kernel,
        out_shape=jax.ShapeDtypeStruct((256, 2048), F32),
        in_specs=[anywhere] * 3,
        out_specs=anywhere,
        scratch_shapes=[
            vm((2, 512, 1024), BF), vm((2, 1024, 2048), BF), vm((4, 512, 512), F32),
            vm((4, 128, 512), BF), vm((4, 128, 512), BF), vm((4, 128, 512), BF),
            vm((4, 128, 512), BF), vm((4, 128, 512), BF), vm((4, 128, 512), BF),
            vm((16, 128, 2048), BF), vm((16, 128, 2048), BF), vm((2, 2, 4, 512, 256), BF),
            vm((2, 512, 2048), BF), vm((4, 1, 2048), F32), vm((4, 1, 2048), F32),
            vm((1, 2048), F32), vm((1, 2048), F32), vm((512, 1), F32),
            vm((128, 1152), F32), vm((128, 1152), BF), vm((4, 32, 1152), BF),
            vm((4, 4, 128, 1152), BF), vm((512, 2048), BF), vm((4, 256, 512), F32),
            pltpu.SemaphoreType.DMA((NSEM,)), pltpu.SemaphoreType.DMA((NSEM,)),
            pltpu.SemaphoreType.DMA((12,)),
        ],
        compiler_params=pltpu.CompilerParams(
            collective_id=0, has_side_effects=True, vmem_limit_bytes=67000000),
        name="vicreg_grad",
    )(hidden_a, hidden_b, weight)


def solution(mesh):
    placed = (P("crop", "dp"), P("crop", "dp"), P("dp", "tensor"))
    return jax.shard_map(
        body, mesh=mesh, in_specs=placed, out_specs=P(("dp", "crop"), "tensor"), check_vma=False
    )
```

```python
import functools

import jax
import jax.numpy as jnp
from jax import lax
from jax.experimental import pallas as pl
from jax.experimental.pallas import tpu as pltpu
from jax.sharding import PartitionSpec as P

MESH = pl.DeviceIdType.MESH
BF, F32 = jnp.bfloat16, jnp.float32
NSEM = 208
VMEM = 58 * 1024 * 1024
EPS = 0.0001
FULL = slice(None)


def mm(a, b, dims=(((1,), (0,)), ((), ()))):
    return lax.dot_general(a, b, dims, preferred_element_type=F32)


def kernel(ha, hb, w, kept, out, hc, wb, acc, s_part, r_part, s_far, s_raw, s_acc, r_far, r_raw, r_acc, zb, cb, hall,
           ht, mx, my, mu, dd, dsum, gf, gb, gr, gp, lt, send, recv, lsem):
    dp = lax.axis_index("dp")
    y = lax.axis_index("crop")
    t = lax.axis_index("tensor")
    x, c = lax.div(dp, 2), lax.rem(dp, 2)
    rows = 2048
    alpha = 50.0 / rows
    cov = 4.0 / (rows - 1.0) ** 2
    sign = jnp.where(c == 0, 1.0, -1.0).astype(F32)

    def turn(v, k):
        return lax.rem(v + k + 4, 4)

    def at_x(k):
        return (2 * turn(x, k) + c, y, t)

    def at_y(k):
        return (dp, turn(y, k), t)

    def at_t(k):
        return (dp, y, turn(t, k))

    partner = (2 * x + 1 - c, y, t)
    count = [0]
    started = []

    def remote(src, dst, dev, index=None):
        if index is None:
            index = count[0]
            count[0] += 1
        return pltpu.make_async_remote_copy(
            src_ref=src, dst_ref=dst, send_sem=send.at[index], recv_sem=recv.at[index],
            device_id=dev, device_id_type=MESH)

    def go(src, dst, dev):
        copy = remote(src, dst, dev)
        copy.start()
        started.append(copy)
        return copy

    def load(src, dst, i):
        return pltpu.make_async_copy(src, dst, lsem.at[i])

    load_h = [load(h, hc.at[v], 4 + v) for v, h in enumerate((ha, hb))]
    load_w = [load(w.at[:, pl.ds(512 * j, 512)], wb.at[:, pl.ds(512 * j, 512)], j) for j in range(4)]
    own = [load(h.at[:, pl.ds(256 * y, 256)], hall.at[v, c, y], 6 + v) for v, h in enumerate((ha, hb))]
    for copy in load_h + load_w + own:
        copy.start()

    barrier = pltpu.get_barrier_semaphore()
    peers = [partner] + [f(k) for f in (at_x, at_y, at_t) for k in (1, 2, 3)]
    for peer in peers:
        pl.semaphore_signal(barrier, inc=1, device_id=peer, device_id_type=MESH)

    def way(j):
        return 1 if j % 2 == 0 else -1

    far, raw, summed = {}, {}, {}

    def rows_of(j, k):
        at = pl.ds(pl.multiple_of(128 * turn(x, k), 128), 128)
        return acc[j, at, :] + r_part[j, at, :].astype(F32)

    def join(j):
        d = way(j)
        part[j].wait_recv()
        s_far[j] = rows_of(j, 2).astype(BF)
        s_raw[j] = rows_of(j, -d).astype(BF)
        far[j] = go(s_far.at[j], r_far.at[j], at_x(d))

    def relay(j):
        d = way(j)
        far[j].wait_recv()
        s_acc[j] = (rows_of(j, d) + r_far[j].astype(F32)).astype(BF)
        summed[j] = go(s_acc.at[j], r_acc.at[j], at_x(d))

    part = []

    def theirs_of(j):
        load_w[j].wait()
        s_part[j] = mm(hc[1 - c], wb[:, 512 * j:512 * j + 512]).astype(BF)

    def give_part(j):
        part.append(go(s_part.at[j], r_part.at[j], partner))

    def ours_of(j):
        acc[j] = mm(hc[c], wb[:, 512 * j:512 * j + 512])

    for copy in load_h:
        copy.wait()
    theirs_of(0)
    pl.semaphore_wait(barrier, len(peers))
    give_part(0)
    theirs_of(1)
    give_part(1)
    ours_of(0)
    join(0)

    def quarter(v):
        return pl.ds(pl.multiple_of(128 * v, 128), 128)

    deal = []
    for k in (1, 3, 2):
        for v, h in enumerate((ha, hb)):
            deal.append((k, v, go(h.at[quarter(t), pl.ds(256 * turn(y, k), 256)], hall.at[v, c, y, quarter(t)], at_y(k))))

    for j in (1, 2, 3):
        if j < 3:
            theirs_of(j + 1)
            give_part(j + 1)
        ours_of(j)
        join(j)

    def send_raw(j):
        raw[j] = go(s_raw.at[j], r_raw.at[j], at_x(-way(j)))

    send_raw(0)
    send_raw(1)
    for j in range(4):
        relay(j)
    send_raw(2)
    send_raw(3)

    block = 4 * y + x

    def settle(j):
        raw[j].wait_recv()
        summed[j].wait_recv()
        cols = slice(512 * j, 512 * j + 512)
        z = (rows_of(j, 0) + r_raw[j].astype(F32) + r_acc[j].astype(F32)).astype(BF)
        zb[block, :, cols] = z
        mx[x, :, cols] = jnp.sum(z.astype(F32), axis=0, keepdims=True)

    split = 896
    cols_of = (pl.ds(0, split), pl.ds(split, 2048 - split))

    class Ring:
        def __init__(self, axis, colour, offset):
            self.axis, self.colour, self.offset = axis, colour, offset
            self.to = at_x if axis == 0 else at_y
            self.right = go(self.piece(0), self.piece(0), self.to(1))
            self.left = go(self.piece(0), self.piece(0), self.to(-1))

        def index(self, k):
            if self.axis == 0:
                return 4 * turn(y, self.offset) + turn(x, k)
            return 4 * turn(y, k) + turn(x, self.offset)

        def piece(self, k, part=pl.ds(0, 128)):
            return zb.at[self.index(k), part, cols_of[self.colour]]

        def take(self):
            low, high = pl.ds(0, 64), pl.ds(64, 64)
            self.right.wait_recv()
            self.on_right = go(self.piece(-1, low), self.piece(-1, low), self.to(1))
            self.left.wait_recv()
            self.on_left = go(self.piece(1, high), self.piece(1, high), self.to(-1))

        def end(self):
            self.on_right.wait_recv()
            self.on_left.wait_recv()

    class Rows:
        def __init__(self, k, v):
            self.slot = hall.at[v, c, turn(y, -k)]
            mine = self.slot.at[quarter(t)]
            self.right, self.left = go(mine, mine, at_t(1)), go(mine, mine, at_t(-1))

        def take(self):
            self.right.wait_recv()
            piece = self.slot.at[pl.ds(pl.multiple_of(128 * turn(t, -1), 128), 64)]
            self.on_right = go(piece, piece, at_t(1))
            self.left.wait_recv()
            piece = self.slot.at[pl.ds(pl.multiple_of(128 * turn(t, 1) + 64, 64), 64)]
            self.on_left = go(piece, piece, at_t(-1))

        def end(self):
            self.on_right.wait_recv()
            self.on_left.wait_recv()

    handed = []
    for v in range(2):
        own[v].wait()
        handed.append(go(hall.at[v, c, y], hall.at[v, c, y], partner))
    spans = []
    for k, v, copy in deal:
        copy.wait_recv()
        spans.append(Rows(k, v))

    settle(0)
    settle(1)
    y_first = Ring(1, 0, 0)
    settle(2)
    settle(3)
    hops = [go(mx.at[x], mx.at[x], at_x(k)) for k in (1, 3, 2)]
    x_first = Ring(0, 1, 0)
    y_rings = {0: Ring(1, 1, 0)}
    x_rings = {0: Ring(0, 0, 0)}
    for hop in hops:
        hop.wait_recv()
    my[y] = mx[0] + mx[1] + mx[2] + mx[3]
    hops = [go(my.at[y], my.at[y], at_y(k)) for k in (1, 3, 2)]
    y_first.take()
    for k in (-1, 1):
        x_rings[k] = Ring(0, 0, k)
    for span in spans:
        span.take()
    x_first.take()
    for k in (-1, 1):
        y_rings[k] = Ring(1, 1, k)
    for span in spans:
        span.end()
        handed.append(go(span.slot, span.slot, partner))
    for hop in hops:
        hop.wait_recv()
    mu[...] = (my[0] + my[1] + my[2] + my[3]) * (1.0 / rows)
    dd[...] = jnp.zeros_like(dd)

    def center(index, colour):
        cols = slice(split * colour, 2048 if colour else split)
        cent = zb[index, :, cols].astype(F32) - mu[:, cols]
        dd[:, cols] += jnp.sum(cent * cent, axis=0, keepdims=True)
        cb[index, :, cols] = cent.astype(BF)

    def center_ring(ring, ks):
        for k in ks:
            center(ring.index(k), ring.colour)

    center(block, 0)
    center(block, 1)
    center_ring(y_first, (-1, 1))
    center_ring(x_first, (-1, 1))
    x_rings[0].take()
    y_rings[0].take()
    y_first.end()
    x_rings[2] = Ring(0, 0, 2)
    x_first.end()
    y_rings[2] = Ring(1, 1, 2)
    center_ring(y_first, (2,))
    center_ring(x_first, (2,))
    center_ring(x_rings[0], (-1, 1))
    center_ring(y_rings[0], (-1, 1))

    def flip(i, _):
        v, r = lax.div(i, 16), lax.rem(i, 16)
        k, yy = lax.div(r, 8), lax.div(lax.rem(r, 8), 2)
        part = lax.rem(r, 2)
        where = pl.multiple_of(512 * yy + 256 * part, 256)
        tile = hall[v, k, yy, pl.ds(pl.multiple_of(256 * part, 256), 256), :]
        ht[v, pl.ds(pl.multiple_of(256 * k, 256), 256), pl.ds(where, 256)] = tile.T
        return 0

    for k in (-1, 1, 2):
        x_rings[k].take()
        y_rings[k].take()
        before_ring = {-1: 0, 1: -1, 2: 1}[k]
        x_rings[before_ring].end()
        y_rings[before_ring].end()
        center_ring(x_rings[before_ring], (2,))
        center_ring(y_rings[before_ring], (2,))
        center_ring(x_rings[k], (-1, 1))
        center_ring(y_rings[k], (-1, 1))
        if k == -1:
            for copy in handed:
                copy.wait_recv()
            lax.fori_loop(0, 16, flip, 0)
        if k == 1:
            lax.fori_loop(16, 32, flip, 0)
        if k == 2:

            def add_up(i, _):
                part = pl.ds(pl.multiple_of(128 * i, 128), 128)
                diff = ht[0, part, :].astype(F32) - ht[1, part, :].astype(F32)
                dsum[part, :] = jnp.sum(diff, axis=1, keepdims=True)
                return 0

            lax.fori_loop(0, 4, add_up, 0)
    x_rings[2].end()
    y_rings[2].end()
    center_ring(x_rings[2], (2,))
    center_ring(y_rings[2], (2,))

    mine = cb[block]

    def strip(v):
        return pl.ds(pl.multiple_of(32 * v, 32), 32)

    sums = []
    for i in range(3):
        cols = pl.ds(384 * i, 384)
        right = jnp.concatenate([cb[lax.rem(block + 3 * i + q, 16)] for q in range(3)], axis=0)
        res = mm(mine, right, (((1,), (1,)), ((), ())))
        gf[:, cols] = res
        gb[:, cols] = res.astype(BF)
        sums.append([go(gb.at[strip(turn(t, k)), cols], gr.at[t, :, cols], at_t(k)) for k in (1, 3, 2)])

    class Turn:
        def __init__(self, axis, colour, done, fixed=None, offset=0):
            self.axis, self.done, self.fixed, self.offset = axis, done, fixed, offset
            self.cols = pl.ds(384 * colour, 384)
            self.to = (at_x, at_y, at_t)[axis]
            self.sent = [go(self.piece(0), self.piece(0), self.to(k)) for k in ((1, -1) if done else (1, -1, 2))]

        def piece(self, k, half=None):
            spots = [x, y, t]
            if self.fixed is not None:
                spots[self.fixed] = turn(spots[self.fixed], self.offset)
            spots[self.axis] = turn(spots[self.axis], k)
            ix, iy, it = spots[0], spots[1], strip(spots[2])
            if half is None:
                whole = {0: pl.ds(0, 4), 1: pl.ds(0, 4), 2: pl.ds(0, 128)}
            else:
                whole = {0: pl.ds(2 * half, 2), 1: pl.ds(2 * half, 2), 2: pl.ds(64 * half, 64)}
            ix = whole[0] if self.done == 0 + 1 else ix
            iy = whole[1] if self.done == 1 + 1 else iy
            it = whole[2] if self.done == 2 + 1 else it
            return gp.at[iy, ix, it, self.cols]

        def take(self):
            self.sent[0].wait_recv()
            self.on_right = go(self.piece(-1, 0), self.piece(-1, 0), self.to(1))
            self.sent[1].wait_recv()
            self.on_left = go(self.piece(1, 1), self.piece(1, 1), self.to(-1))

        def end(self):
            self.on_right.wait_recv()
            self.on_left.wait_recv()

    orders = ((2, 1, 0), (0, 2, 1), (1, 0, 2))

    firsts = []
    for i, order in enumerate(orders):
        cols = pl.ds(384 * i, 384)
        for hop in sums[i]:
            hop.wait_recv()
        total = gf[strip(t), cols]
        for k in (1, 2, 3):
            total = total + gr[turn(t, k), :, cols].astype(F32)
        gp[y, x, strip(t), cols] = total.astype(BF)
        firsts.append(Turn(order[0], i, 0))

    spread = dd[...]
    dev = jnp.sqrt(spread * (1.0 / (rows - 1.0)) + EPS)
    rate = jnp.where(dev < 1.0, 25.0 / ((rows - 1.0) * dev), 0.0) + cov * spread
    dd[...] = rate

    def plain(n, _):
        j, p = lax.div(n, 2), lax.rem(n, 2)
        cols = pl.ds(pl.multiple_of(256 * n, 256), 256)
        at = pl.ds(pl.multiple_of(256 * p, 256), 256)
        right = cb[:, :, cols].reshape(2048, 256)
        acc[j, :, at] = (sign * alpha) * dsum[...] * mu[:, cols] - mm(ht[c], right) * dd[:, cols]
        return 0

    lax.fori_loop(0, 2, plain, 0)
    for first in firsts:
        for copy in first.sent:
            copy.wait_recv()
    seconds = [Turn(b, i, a + 1) for i, (a, b, d) in enumerate(orders)]

    def third(offset):
        return [Turn(d, i, a + 1, b, offset) for i, (a, b, d) in enumerate(orders)]

    def take(turns):
        for one in turns:
            one.take()

    def end(turns):
        for one in turns:
            one.end()

    thirds = {0: third(0)}
    lax.fori_loop(2, 4, plain, 0)
    take(seconds)
    thirds[-1] = third(-1)
    thirds[1] = third(1)
    take(thirds[0])
    lax.fori_loop(4, 6, plain, 0)
    end(seconds)
    thirds[2] = third(2)
    lax.fori_loop(6, 7, plain, 0)
    take(thirds[-1])
    end(thirds[0])
    take(thirds[1])
    lax.fori_loop(7, 8, plain, 0)
    take(thirds[2])
    for offset in (-1, 1, 2):
        end(thirds[offset])

    for copy in started:
        copy.wait_send()
    started.clear()

    def spread_panel(b, _):
        by, bx = lax.div(b, 4), lax.rem(b, 4)
        here = pl.ds(pl.multiple_of(128 * b, 128), 128)
        for j in range(9):
            other = lax.rem(b + j, 16)
            tile = gp[by, bx, :, 128 * j:128 * j + 128]
            zb[b, :, pl.ds(pl.multiple_of(128 * other, 128), 128)] = tile
            if 0 < j < 8:
                zb[other, :, here] = tile.T
        return 0

    lax.fori_loop(0, 16, spread_panel, 0)

    def factor(n, _):
        cols = pl.ds(pl.multiple_of(512 * n, 512), 512)
        res = mm(ht[c], zb[:, :, cols].reshape(2048, 512))
        diff = ht[0, :, cols].astype(F32) - ht[1, :, cols].astype(F32)
        lt[:, cols] = (cov * res + (sign * alpha) * diff).astype(BF)
        return 0

    lax.fori_loop(0, 4, factor, 0)

    theirs = pl.ds(pl.multiple_of(256 * (1 - c), 256), 256)
    ours = pl.ds(pl.multiple_of(256 * c, 256), 256)

    spots = ((0, 0, 512), (1, 0, 512), (2, 0, 512), (3, 0, 256), (3, 256, 256))
    give, stores = [], []

    for n, (j, low, wide) in enumerate(spots):
        at = pl.ds(low, wide)
        where = pl.ds(512 * j + low, wide)
        right = cb[:, :, 512 * j + low:512 * j + low + wide].reshape(2048, wide)
        acc[j, :, at] += mm(lt[...], right)
        give.append(go(acc.at[j, theirs, at], out.at[:, where], partner))
        stores.append(load(acc.at[j, ours, at], kept.at[:, where], 8 + n))
        stores[n].start()
    for copy in give:
        copy.wait_recv()
    for copy in started:
        copy.wait_send()
    for copy in stores:
        copy.wait()


def body(hidden_a, hidden_b, weight):
    anywhere = pl.BlockSpec(memory_space=pl.ANY)
    vm = pltpu.VMEM
    kept, given = pl.pallas_call(
        kernel,
        out_shape=[jax.ShapeDtypeStruct((256, 2048), F32)] * 2,
        in_specs=[anywhere] * 3,
        out_specs=[anywhere] * 2,
        scratch_shapes=[
            vm((2, 512, 1024), BF), vm((1024, 2048), BF), vm((4, 512, 512), F32),
            vm((4, 512, 512), BF), vm((4, 512, 512), BF),
            vm((4, 128, 512), BF), vm((4, 128, 512), BF), vm((4, 128, 512), BF),
            vm((4, 128, 512), BF), vm((4, 128, 512), BF), vm((4, 128, 512), BF),
            vm((16, 128, 2048), BF), vm((16, 128, 2048), BF), vm((2, 2, 4, 512, 256), BF),
            vm((2, 512, 2048), BF), vm((4, 1, 2048), F32), vm((4, 1, 2048), F32),
            vm((1, 2048), F32), vm((1, 2048), F32), vm((512, 1), F32),
            vm((128, 1152), F32), vm((128, 1152), BF), vm((4, 32, 1152), BF),
            vm((4, 4, 128, 1152), BF), vm((512, 2048), BF),
            pltpu.SemaphoreType.DMA((NSEM,)), pltpu.SemaphoreType.DMA((NSEM,)),
            pltpu.SemaphoreType.DMA((16,)),
        ],
        compiler_params=pltpu.CompilerParams(
            collective_id=0, has_side_effects=True, vmem_limit_bytes=VMEM),
        name="vicreg_grad",
    )(hidden_a, hidden_b, weight)
    return kept + given


def solution(mesh):
    placed = (P("crop", "dp"), P("crop", "dp"), P("dp", "tensor"))
    return jax.shard_map(
        body, mesh=mesh, in_specs=placed, out_specs=P(("dp", "crop"), "tensor"), check_vma=False
    )
```

```python
import functools

import jax
import jax.numpy as jnp
from jax import lax
from jax.experimental import pallas as pl
from jax.experimental.pallas import tpu as pltpu
from jax.sharding import PartitionSpec as P

MESH = pl.DeviceIdType.MESH
BF, F32 = jnp.bfloat16, jnp.float32
NSEM = 208
VMEM = 58 * 1024 * 1024
EPS = 0.0001
FULL = slice(None)


def mm(a, b, dims=(((1,), (0,)), ((), ()))):
    return lax.dot_general(a, b, dims, preferred_element_type=F32)


def kernel(ha, hb, w, kept, out, hc, wb, acc, s_part, r_part, s_far, s_raw, s_acc, r_far, r_raw, r_acc, zb, cb, hall,
           ht, mx, my, mu, dd, dsum, gf, gb, gr, gp, lt, send, recv, lsem):
    dp = lax.axis_index("dp")
    y = lax.axis_index("crop")
    t = lax.axis_index("tensor")
    x, c = lax.div(dp, 2), lax.rem(dp, 2)
    rows = 2048
    alpha = 50.0 / rows
    cov = 4.0 / (rows - 1.0) ** 2
    sign = jnp.where(c == 0, 1.0, -1.0).astype(F32)

    def turn(v, k):
        return lax.rem(v + k + 4, 4)

    def at_x(k):
        return (2 * turn(x, k) + c, y, t)

    def at_y(k):
        return (dp, turn(y, k), t)

    def at_t(k):
        return (dp, y, turn(t, k))

    partner = (2 * x + 1 - c, y, t)
    count = [0]
    started = []

    def remote(src, dst, dev, index=None):
        if index is None:
            index = count[0]
            count[0] += 1
        return pltpu.make_async_remote_copy(
            src_ref=src, dst_ref=dst, send_sem=send.at[index], recv_sem=recv.at[index],
            device_id=dev, device_id_type=MESH)

    def go(src, dst, dev):
        copy = remote(src, dst, dev)
        copy.start()
        started.append(copy)
        return copy

    def load(src, dst, i):
        return pltpu.make_async_copy(src, dst, lsem.at[i])

    load_h = [load(h, hc.at[v], 4 + v) for v, h in enumerate((ha, hb))]
    load_w = [load(w.at[:, pl.ds(512 * j, 512)], wb.at[:, pl.ds(512 * j, 512)], j) for j in range(4)]
    own = [load(h.at[:, pl.ds(256 * y, 256)], hall.at[v, c, y], 6 + v) for v, h in enumerate((ha, hb))]
    for copy in load_h + load_w + own:
        copy.start()

    barrier = pltpu.get_barrier_semaphore()
    peers = [partner] + [f(k) for f in (at_x, at_y, at_t) for k in (1, 2, 3)]
    for peer in peers:
        pl.semaphore_signal(barrier, inc=1, device_id=peer, device_id_type=MESH)

    def way(j):
        return 1 if j % 2 == 0 else -1

    far, raw, summed = {}, {}, {}

    def rows_of(j, k):
        at = pl.ds(pl.multiple_of(128 * turn(x, k), 128), 128)
        return acc[j, at, :] + r_part[j, at, :].astype(F32)

    def join(j):
        d = way(j)
        part[j].wait_recv()
        s_far[j] = rows_of(j, 2).astype(BF)
        s_raw[j] = rows_of(j, -d).astype(BF)
        far[j] = go(s_far.at[j], r_far.at[j], at_x(d))

    def relay(j):
        d = way(j)
        far[j].wait_recv()
        s_acc[j] = (rows_of(j, d) + r_far[j].astype(F32)).astype(BF)
        summed[j] = go(s_acc.at[j], r_acc.at[j], at_x(d))

    part = []

    def theirs_of(j):
        load_w[j].wait()
        s_part[j] = mm(hc[1 - c], wb[:, 512 * j:512 * j + 512]).astype(BF)

    def give_part(j):
        part.append(go(s_part.at[j], r_part.at[j], partner))

    def ours_of(j):
        acc[j] = mm(hc[c], wb[:, 512 * j:512 * j + 512])

    for copy in load_h:
        copy.wait()
    theirs_of(0)
    pl.semaphore_wait(barrier, len(peers))
    give_part(0)
    theirs_of(1)
    give_part(1)
    ours_of(0)
    join(0)

    def quarter(v):
        return pl.ds(pl.multiple_of(128 * v, 128), 128)

    deal = []
    for k in (1, 3, 2):
        for v, h in enumerate((ha, hb)):
            deal.append((k, v, go(h.at[quarter(t), pl.ds(256 * turn(y, k), 256)], hall.at[v, c, y, quarter(t)], at_y(k))))

    ours_of(1)
    join(1)

    def send_raw(j):
        raw[j] = go(s_raw.at[j], r_raw.at[j], at_x(-way(j)))

    send_raw(0)
    send_raw(1)
    for j in (2, 3):
        theirs_of(j)
        give_part(j)
    for j in (2, 3):
        ours_of(j)
    relay(0)
    relay(1)
    join(2)
    join(3)
    send_raw(2)
    send_raw(3)
    relay(2)
    relay(3)

    block = 4 * y + x

    def settle(j):
        raw[j].wait_recv()
        summed[j].wait_recv()
        cols = slice(512 * j, 512 * j + 512)
        z = (rows_of(j, 0) + r_raw[j].astype(F32) + r_acc[j].astype(F32)).astype(BF)
        zb[block, :, cols] = z
        mx[x, :, cols] = jnp.sum(z.astype(F32), axis=0, keepdims=True)

    split = 896
    cols_of = (pl.ds(0, split), pl.ds(split, 2048 - split))

    class Ring:
        def __init__(self, axis, colour, offset):
            self.axis, self.colour, self.offset = axis, colour, offset
            self.to = at_x if axis == 0 else at_y
            self.right = go(self.piece(0), self.piece(0), self.to(1))
            self.left = go(self.piece(0), self.piece(0), self.to(-1))

        def index(self, k):
            if self.axis == 0:
                return 4 * turn(y, self.offset) + turn(x, k)
            return 4 * turn(y, k) + turn(x, self.offset)

        def piece(self, k, part=pl.ds(0, 128)):
            return zb.at[self.index(k), part, cols_of[self.colour]]

        def take(self):
            low, high = pl.ds(0, 64), pl.ds(64, 64)
            self.right.wait_recv()
            self.on_right = go(self.piece(-1, low), self.piece(-1, low), self.to(1))
            self.left.wait_recv()
            self.on_left = go(self.piece(1, high), self.piece(1, high), self.to(-1))

        def end(self):
            self.on_right.wait_recv()
            self.on_left.wait_recv()

    class Rows:
        def __init__(self, k, v):
            self.slot = hall.at[v, c, turn(y, -k)]
            mine = self.slot.at[quarter(t)]
            self.right, self.left = go(mine, mine, at_t(1)), go(mine, mine, at_t(-1))

        def take(self):
            self.right.wait_recv()
            piece = self.slot.at[pl.ds(pl.multiple_of(128 * turn(t, -1), 128), 64)]
            self.on_right = go(piece, piece, at_t(1))
            self.left.wait_recv()
            piece = self.slot.at[pl.ds(pl.multiple_of(128 * turn(t, 1) + 64, 64), 64)]
            self.on_left = go(piece, piece, at_t(-1))

        def end(self):
            self.on_right.wait_recv()
            self.on_left.wait_recv()

    handed = []
    for v in range(2):
        own[v].wait()
        handed.append(go(hall.at[v, c, y], hall.at[v, c, y], partner))
    spans = []
    for k, v, copy in deal:
        copy.wait_recv()
        spans.append(Rows(k, v))

    settle(0)
    settle(1)
    y_first = Ring(1, 0, 0)
    settle(2)
    settle(3)
    hops = [go(mx.at[x], mx.at[x], at_x(k)) for k in (1, 3, 2)]
    x_first = Ring(0, 1, 0)
    y_rings = {0: Ring(1, 1, 0)}
    x_rings = {0: Ring(0, 0, 0)}
    for hop in hops:
        hop.wait_recv()
    my[y] = mx[0] + mx[1] + mx[2] + mx[3]
    hops = [go(my.at[y], my.at[y], at_y(k)) for k in (1, 3, 2)]
    y_first.take()
    for k in (-1, 1):
        x_rings[k] = Ring(0, 0, k)
    for span in spans:
        span.take()
    x_first.take()
    for k in (-1, 1):
        y_rings[k] = Ring(1, 1, k)
    for span in spans:
        span.end()
        handed.append(go(span.slot, span.slot, partner))
    for hop in hops:
        hop.wait_recv()
    mu[...] = (my[0] + my[1] + my[2] + my[3]) * (1.0 / rows)
    dd[...] = jnp.zeros_like(dd)

    def center(index, colour):
        cols = slice(split * colour, 2048 if colour else split)
        cent = zb[index, :, cols].astype(F32) - mu[:, cols]
        dd[:, cols] += jnp.sum(cent * cent, axis=0, keepdims=True)
        cb[index, :, cols] = cent.astype(BF)

    def center_ring(ring, ks):
        for k in ks:
            center(ring.index(k), ring.colour)

    x_rings[0].take()
    y_rings[0].take()
    center(block, 0)
    center(block, 1)
    center_ring(y_first, (-1, 1))
    center_ring(x_first, (-1, 1))
    y_first.end()
    x_rings[2] = Ring(0, 0, 2)
    x_first.end()
    y_rings[2] = Ring(1, 1, 2)

    def flip(i, _):
        v, r = lax.div(i, 16), lax.rem(i, 16)
        k, yy = lax.div(r, 8), lax.div(lax.rem(r, 8), 2)
        part = lax.rem(r, 2)
        where = pl.multiple_of(512 * yy + 256 * part, 256)
        tile = hall[v, k, yy, pl.ds(pl.multiple_of(256 * part, 256), 256), :]
        ht[v, pl.ds(pl.multiple_of(256 * k, 256), 256), pl.ds(where, 256)] = tile.T
        return 0

    def add_up(i, _):
        at = pl.ds(pl.multiple_of(128 * i, 128), 128)
        diff = ht[0, at, :].astype(F32) - ht[1, at, :].astype(F32)
        dsum[at, :] = jnp.sum(diff, axis=1, keepdims=True)
        return 0

    center_ring(y_first, (2,))
    center_ring(x_first, (2,))
    center_ring(x_rings[0], (-1, 1))
    center_ring(y_rings[0], (-1, 1))
    for k in (-1, 1):
        x_rings[k].take()
        y_rings[k].take()
    for copy in handed:
        copy.wait_recv()
    lax.fori_loop(0, 16, flip, 0)
    x_rings[0].end()
    y_rings[0].end()
    center_ring(x_rings[0], (2,))
    center_ring(y_rings[0], (2,))
    x_rings[2].take()
    y_rings[2].take()
    for k in (-1, 1):
        center_ring(x_rings[k], (-1, 1))
        center_ring(y_rings[k], (-1, 1))
    lax.fori_loop(16, 32, flip, 0)
    lax.fori_loop(0, 4, add_up, 0)
    center_ring(x_rings[2], (-1, 1))
    center_ring(y_rings[2], (-1, 1))
    for k in (-1, 1, 2):
        x_rings[k].end()
        center_ring(x_rings[k], (2,))
        y_rings[k].end()
        center_ring(y_rings[k], (2,))

    mine = cb[block]

    def strip(v):
        return pl.ds(pl.multiple_of(32 * v, 32), 32)

    sums = []
    for p, i in enumerate((None, 0, 1, None, 2)):
        wide = 256 if p < 4 else 128
        right = cb[lax.rem(block + 2 * p, 16)]
        if p < 4:
            right = jnp.concatenate([right, cb[lax.rem(block + 2 * p + 1, 16)]], axis=0)
        res = mm(mine, right, (((1,), (1,)), ((), ())))
        gf[:, 256 * p:256 * p + wide] = res
        gb[:, 256 * p:256 * p + wide] = res.astype(BF)
        if i is not None:
            cols = pl.ds(384 * i, 384)
            sums.append([go(gb.at[strip(turn(t, k)), cols], gr.at[t, :, cols], at_t(k)) for k in (1, 3, 2)])

    class Turn:
        def __init__(self, axis, colour, done, fixed=None, offset=0):
            self.axis, self.done, self.fixed, self.offset = axis, done, fixed, offset
            self.cols = pl.ds(384 * colour, 384)
            self.to = (at_x, at_y, at_t)[axis]
            self.sent = [go(self.piece(0), self.piece(0), self.to(k)) for k in ((1, -1) if done else (1, -1, 2))]

        def piece(self, k, half=None):
            spots = [x, y, t]
            if self.fixed is not None:
                spots[self.fixed] = turn(spots[self.fixed], self.offset)
            spots[self.axis] = turn(spots[self.axis], k)
            ix, iy, it = spots[0], spots[1], strip(spots[2])
            if half is None:
                whole = {0: pl.ds(0, 4), 1: pl.ds(0, 4), 2: pl.ds(0, 128)}
            else:
                whole = {0: pl.ds(2 * half, 2), 1: pl.ds(2 * half, 2), 2: pl.ds(64 * half, 64)}
            ix = whole[0] if self.done == 0 + 1 else ix
            iy = whole[1] if self.done == 1 + 1 else iy
            it = whole[2] if self.done == 2 + 1 else it
            return gp.at[iy, ix, it, self.cols]

        def take(self):
            self.sent[0].wait_recv()
            self.on_right = go(self.piece(-1, 0), self.piece(-1, 0), self.to(1))
            self.sent[1].wait_recv()
            self.on_left = go(self.piece(1, 1), self.piece(1, 1), self.to(-1))

        def end(self):
            self.on_right.wait_recv()
            self.on_left.wait_recv()

    orders = ((2, 1, 0), (0, 2, 1), (1, 0, 2))

    firsts = []
    for i, order in enumerate(orders):
        cols = pl.ds(384 * i, 384)
        for hop in sums[i]:
            hop.wait_recv()
        total = gf[strip(t), cols]
        for k in (1, 2, 3):
            total = total + gr[turn(t, k), :, cols].astype(F32)
        gp[y, x, strip(t), cols] = total.astype(BF)
        firsts.append(Turn(order[0], i, 0))

    spread = dd[...]
    dev = jnp.sqrt(spread * (1.0 / (rows - 1.0)) + EPS)
    rate = jnp.where(dev < 1.0, 25.0 / ((rows - 1.0) * dev), 0.0) + cov * spread
    dd[...] = rate

    def plain(n, _):
        j, p = lax.div(n, 2), lax.rem(n, 2)
        cols = pl.ds(pl.multiple_of(256 * n, 256), 256)
        at = pl.ds(pl.multiple_of(256 * p, 256), 256)
        right = cb[:, :, cols].reshape(2048, 256)
        acc[j, :, at] = (sign * alpha) * dsum[...] * mu[:, cols] - mm(ht[c], right) * dd[:, cols]
        return 0

    lax.fori_loop(0, 2, plain, 0)
    for first in firsts:
        for copy in first.sent:
            copy.wait_recv()
    seconds = [Turn(b, i, a + 1) for i, (a, b, d) in enumerate(orders)]

    def third(offset):
        return [Turn(d, i, a + 1, b, offset) for i, (a, b, d) in enumerate(orders)]

    def take(turns):
        for one in turns:
            one.take()

    def end(turns):
        for one in turns:
            one.end()

    thirds = {0: third(0)}
    lax.fori_loop(2, 5, plain, 0)
    take(seconds)
    thirds[-1] = third(-1)
    thirds[1] = third(1)
    take(thirds[0])
    end(seconds)
    thirds[2] = third(2)
    lax.fori_loop(5, 8, plain, 0)
    take(thirds[-1])
    take(thirds[1])
    take(thirds[2])
    for offset in (0, -1, 1, 2):
        end(thirds[offset])

    for copy in started:
        copy.wait_send()
    started.clear()

    def spread_panel(b, _):
        by, bx = lax.div(b, 4), lax.rem(b, 4)
        here = pl.ds(pl.multiple_of(128 * b, 128), 128)
        for j in range(9):
            other = lax.rem(b + j, 16)
            tile = gp[by, bx, :, 128 * j:128 * j + 128]
            zb[b, :, pl.ds(pl.multiple_of(128 * other, 128), 128)] = tile
            if 0 < j < 8:
                zb[other, :, here] = tile.T
        return 0

    lax.fori_loop(0, 16, spread_panel, 0)

    def factor(n, _):
        cols = pl.ds(pl.multiple_of(512 * n, 512), 512)
        res = mm(ht[c], zb[:, :, cols].reshape(2048, 512))
        diff = ht[0, :, cols].astype(F32) - ht[1, :, cols].astype(F32)
        lt[:, cols] = (cov * res + (sign * alpha) * diff).astype(BF)
        return 0

    lax.fori_loop(0, 4, factor, 0)

    theirs = pl.ds(pl.multiple_of(256 * (1 - c), 256), 256)
    ours = pl.ds(pl.multiple_of(256 * c, 256), 256)

    spots = ((0, 0, 512), (1, 0, 512), (2, 0, 512), (3, 0, 256), (3, 256, 256))
    give, stores = [], []

    for n, (j, low, wide) in enumerate(spots):
        at = pl.ds(low, wide)
        where = pl.ds(512 * j + low, wide)
        right = cb[:, :, 512 * j + low:512 * j + low + wide].reshape(2048, wide)
        acc[j, :, at] += mm(lt[...], right)
        give.append(go(acc.at[j, theirs, at], out.at[:, where], partner))
        stores.append(load(acc.at[j, ours, at], kept.at[:, where], 8 + n))
        stores[n].start()
    for copy in give:
        copy.wait_recv()
    for copy in started:
        copy.wait_send()
    for copy in stores:
        copy.wait()


def body(hidden_a, hidden_b, weight):
    anywhere = pl.BlockSpec(memory_space=pl.ANY)
    vm = pltpu.VMEM
    kept, given = pl.pallas_call(
        kernel,
        out_shape=[jax.ShapeDtypeStruct((256, 2048), F32)] * 2,
        in_specs=[anywhere] * 3,
        out_specs=[anywhere] * 2,
        scratch_shapes=[
            vm((2, 512, 1024), BF), vm((1024, 2048), BF), vm((4, 512, 512), F32),
            vm((4, 512, 512), BF), vm((4, 512, 512), BF),
            vm((4, 128, 512), BF), vm((4, 128, 512), BF), vm((4, 128, 512), BF),
            vm((4, 128, 512), BF), vm((4, 128, 512), BF), vm((4, 128, 512), BF),
            vm((16, 128, 2048), BF), vm((16, 128, 2048), BF), vm((2, 2, 4, 512, 256), BF),
            vm((2, 512, 2048), BF), vm((4, 1, 2048), F32), vm((4, 1, 2048), F32),
            vm((1, 2048), F32), vm((1, 2048), F32), vm((512, 1), F32),
            vm((128, 1152), F32), vm((128, 1152), BF), vm((4, 32, 1152), BF),
            vm((4, 4, 128, 1152), BF), vm((512, 2048), BF),
            pltpu.SemaphoreType.DMA((NSEM,)), pltpu.SemaphoreType.DMA((NSEM,)),
            pltpu.SemaphoreType.DMA((16,)),
        ],
        compiler_params=pltpu.CompilerParams(
            collective_id=0, has_side_effects=True, vmem_limit_bytes=VMEM),
        name="vicreg_grad",
    )(hidden_a, hidden_b, weight)
    return kept + given


def solution(mesh):
    placed = (P("crop", "dp"), P("crop", "dp"), P("dp", "tensor"))
    return jax.shard_map(
        body, mesh=mesh, in_specs=placed, out_specs=P(("dp", "crop"), "tensor"), check_vma=False
    )
```

```python
import functools

import jax
import jax.numpy as jnp
from jax import lax
from jax.experimental import pallas as pl
from jax.experimental.pallas import tpu as pltpu
from jax.sharding import PartitionSpec as P

MESH = pl.DeviceIdType.MESH
BF, F32 = jnp.bfloat16, jnp.float32
NSEM = 208
VMEM = 58 * 1024 * 1024
EPS = 0.0001
FULL = slice(None)


def mm(a, b, dims=(((1,), (0,)), ((), ()))):
    return lax.dot_general(a, b, dims, preferred_element_type=F32)


def kernel(ha, hb, w, kept, out, hc, wb, acc, s_part, r_part, s_far, s_raw, s_acc, r_far, r_raw, r_acc, zb, cb, hall,
           ht, mx, my, mu, dd, dsum, gf, gb, gr, gp, lt, send, recv, lsem):
    dp = lax.axis_index("dp")
    y = lax.axis_index("crop")
    t = lax.axis_index("tensor")
    x, c = lax.div(dp, 2), lax.rem(dp, 2)
    rows = 2048
    alpha = 50.0 / rows
    cov = 4.0 / (rows - 1.0) ** 2
    sign = jnp.where(c == 0, 1.0, -1.0).astype(F32)

    def turn(v, k):
        return lax.rem(v + k + 4, 4)

    def at_x(k):
        return (2 * turn(x, k) + c, y, t)

    def at_y(k):
        return (dp, turn(y, k), t)

    def at_t(k):
        return (dp, y, turn(t, k))

    partner = (2 * x + 1 - c, y, t)
    count = [0]
    started = []

    def remote(src, dst, dev, index=None):
        if index is None:
            index = count[0]
            count[0] += 1
        return pltpu.make_async_remote_copy(
            src_ref=src, dst_ref=dst, send_sem=send.at[index], recv_sem=recv.at[index],
            device_id=dev, device_id_type=MESH)

    def go(src, dst, dev):
        copy = remote(src, dst, dev)
        copy.start()
        started.append(copy)
        return copy

    def load(src, dst, i):
        return pltpu.make_async_copy(src, dst, lsem.at[i])

    load_h = [load(h, hc.at[v], 4 + v) for v, h in enumerate((ha, hb))]
    load_w = [load(w.at[:, pl.ds(512 * j, 512)], wb.at[:, pl.ds(512 * j, 512)], j) for j in range(4)]
    own = [load(h.at[:, pl.ds(256 * y, 256)], hall.at[v, c, y], 6 + v) for v, h in enumerate((ha, hb))]
    for copy in load_h + load_w + own:
        copy.start()

    barrier = pltpu.get_barrier_semaphore()
    peers = [partner] + [f(k) for f in (at_x, at_y, at_t) for k in (1, 2, 3)]
    for peer in peers:
        pl.semaphore_signal(barrier, inc=1, device_id=peer, device_id_type=MESH)

    def way(j):
        return 1 if j % 2 == 0 else -1

    far, raw, summed = {}, {}, {}

    def rows_of(j, k):
        at = pl.ds(pl.multiple_of(128 * turn(x, k), 128), 128)
        return acc[j, at, :] + r_part[j, at, :].astype(F32)

    def join(j):
        d = way(j)
        part[j].wait_recv()
        s_far[j] = rows_of(j, 2).astype(BF)
        s_raw[j] = rows_of(j, -d).astype(BF)
        far[j] = go(s_far.at[j], r_far.at[j], at_x(d))

    def relay(j):
        d = way(j)
        far[j].wait_recv()
        s_acc[j] = (rows_of(j, d) + r_far[j].astype(F32)).astype(BF)
        summed[j] = go(s_acc.at[j], r_acc.at[j], at_x(d))

    part = []

    def theirs_of(j):
        load_w[j].wait()
        s_part[j] = mm(hc[1 - c], wb[:, 512 * j:512 * j + 512]).astype(BF)

    def give_part(j):
        part.append(go(s_part.at[j], r_part.at[j], partner))

    def ours_of(j):
        acc[j] = mm(hc[c], wb[:, 512 * j:512 * j + 512])

    for copy in load_h:
        copy.wait()
    theirs_of(0)
    pl.semaphore_wait(barrier, len(peers))
    give_part(0)
    theirs_of(1)
    give_part(1)
    ours_of(0)
    join(0)

    def quarter(v):
        return pl.ds(pl.multiple_of(128 * v, 128), 128)

    deal = []
    for k in (1, 3, 2):
        for v, h in enumerate((ha, hb)):
            deal.append((k, v, go(h.at[quarter(t), pl.ds(256 * turn(y, k), 256)], hall.at[v, c, y, quarter(t)], at_y(k))))

    ours_of(1)
    join(1)

    def send_raw(j):
        raw[j] = go(s_raw.at[j], r_raw.at[j], at_x(-way(j)))

    send_raw(0)
    send_raw(1)
    for j in (2, 3):
        theirs_of(j)
        give_part(j)
    for j in (2, 3):
        ours_of(j)
    relay(0)
    relay(1)
    join(2)
    join(3)
    send_raw(2)
    send_raw(3)
    relay(2)
    relay(3)

    block = 4 * y + x

    def settle(j):
        raw[j].wait_recv()
        summed[j].wait_recv()
        cols = slice(512 * j, 512 * j + 512)
        z = (rows_of(j, 0) + r_raw[j].astype(F32) + r_acc[j].astype(F32)).astype(BF)
        zb[block, :, cols] = z
        mx[x, :, cols] = jnp.sum(z.astype(F32), axis=0, keepdims=True)

    split = 896
    cols_of = (pl.ds(0, split), pl.ds(split, 2048 - split))

    class Ring:
        def __init__(self, axis, colour, offset):
            self.axis, self.colour, self.offset = axis, colour, offset
            self.to = at_x if axis == 0 else at_y
            self.right = go(self.piece(0), self.piece(0), self.to(1))
            self.left = go(self.piece(0), self.piece(0), self.to(-1))

        def index(self, k):
            if self.axis == 0:
                return 4 * turn(y, self.offset) + turn(x, k)
            return 4 * turn(y, k) + turn(x, self.offset)

        def piece(self, k, part=pl.ds(0, 128)):
            return zb.at[self.index(k), part, cols_of[self.colour]]

        def take(self):
            low, high = pl.ds(0, 64), pl.ds(64, 64)
            self.right.wait_recv()
            self.on_right = go(self.piece(-1, low), self.piece(-1, low), self.to(1))
            self.left.wait_recv()
            self.on_left = go(self.piece(1, high), self.piece(1, high), self.to(-1))

        def end(self):
            self.on_right.wait_recv()
            self.on_left.wait_recv()

    class Rows:
        def __init__(self, k, v):
            self.slot = hall.at[v, c, turn(y, -k)]
            mine = self.slot.at[quarter(t)]
            self.right, self.left = go(mine, mine, at_t(1)), go(mine, mine, at_t(-1))

        def take(self):
            self.right.wait_recv()
            piece = self.slot.at[pl.ds(pl.multiple_of(128 * turn(t, -1), 128), 64)]
            self.on_right = go(piece, piece, at_t(1))
            self.left.wait_recv()
            piece = self.slot.at[pl.ds(pl.multiple_of(128 * turn(t, 1) + 64, 64), 64)]
            self.on_left = go(piece, piece, at_t(-1))

        def end(self):
            self.on_right.wait_recv()
            self.on_left.wait_recv()

    handed = []
    for v in range(2):
        own[v].wait()
        handed.append(go(hall.at[v, c, y], hall.at[v, c, y], partner))
    spans = []
    for k, v, copy in deal:
        copy.wait_recv()
        spans.append(Rows(k, v))

    settle(0)
    settle(1)
    y_first = Ring(1, 0, 0)
    settle(2)
    settle(3)
    hops = [go(mx.at[x], mx.at[x], at_x(k)) for k in (1, 3, 2)]
    x_first = Ring(0, 1, 0)
    y_rings = {0: Ring(1, 1, 0)}
    x_rings = {0: Ring(0, 0, 0)}
    for hop in hops:
        hop.wait_recv()
    my[y] = mx[0] + mx[1] + mx[2] + mx[3]
    hops = [go(my.at[y], my.at[y], at_y(k)) for k in (1, 3, 2)]
    y_first.take()
    for k in (-1, 1):
        x_rings[k] = Ring(0, 0, k)
    for span in spans:
        span.take()
    x_first.take()
    for k in (-1, 1):
        y_rings[k] = Ring(1, 1, k)
    for span in spans:
        span.end()
        handed.append(go(span.slot, span.slot, partner))
    for hop in hops:
        hop.wait_recv()
    mu[...] = (my[0] + my[1] + my[2] + my[3]) * (1.0 / rows)
    dd[...] = jnp.zeros_like(dd)

    def center(index, colour):
        cols = slice(split * colour, 2048 if colour else split)
        cent = zb[index, :, cols].astype(F32) - mu[:, cols]
        dd[:, cols] += jnp.sum(cent * cent, axis=0, keepdims=True)
        cb[index, :, cols] = cent.astype(BF)

    def center_ring(ring, ks):
        for k in ks:
            center(ring.index(k), ring.colour)

    x_rings[0].take()
    y_rings[0].take()
    center(block, 0)
    center(block, 1)
    center_ring(y_first, (-1, 1))
    center_ring(x_first, (-1, 1))
    y_first.end()
    x_rings[2] = Ring(0, 0, 2)
    x_first.end()
    y_rings[2] = Ring(1, 1, 2)

    def flip(i, _):
        v, r = lax.div(i, 16), lax.rem(i, 16)
        k, yy = lax.div(r, 8), lax.div(lax.rem(r, 8), 2)
        part = lax.rem(r, 2)
        where = pl.multiple_of(512 * yy + 256 * part, 256)
        tile = hall[v, k, yy, pl.ds(pl.multiple_of(256 * part, 256), 256), :]
        ht[v, pl.ds(pl.multiple_of(256 * k, 256), 256), pl.ds(where, 256)] = tile.T
        return 0

    def add_up(i, _):
        at = pl.ds(pl.multiple_of(128 * i, 128), 128)
        diff = ht[0, at, :].astype(F32) - ht[1, at, :].astype(F32)
        dsum[at, :] = jnp.sum(diff, axis=1, keepdims=True)
        return 0

    center_ring(y_first, (2,))
    center_ring(x_first, (2,))
    center_ring(x_rings[0], (-1, 1))
    center_ring(y_rings[0], (-1, 1))
    for k in (-1, 1):
        x_rings[k].take()
        y_rings[k].take()
    for copy in handed:
        copy.wait_recv()
    lax.fori_loop(0, 16, flip, 0)
    x_rings[0].end()
    y_rings[0].end()
    center_ring(x_rings[0], (2,))
    center_ring(y_rings[0], (2,))
    x_rings[2].take()
    y_rings[2].take()
    for k in (-1, 1):
        center_ring(x_rings[k], (-1, 1))
        center_ring(y_rings[k], (-1, 1))
    lax.fori_loop(16, 32, flip, 0)
    lax.fori_loop(0, 4, add_up, 0)
    center_ring(x_rings[2], (-1, 1))
    center_ring(y_rings[2], (-1, 1))
    for k in (-1, 1, 2):
        x_rings[k].end()
        center_ring(x_rings[k], (2,))
        y_rings[k].end()
        center_ring(y_rings[k], (2,))

    mine = cb[block]

    def strip(v):
        return pl.ds(pl.multiple_of(32 * v, 32), 32)

    early = list(started)
    started.clear()
    sums = []
    for p, i in enumerate((None, 0, 1, None, 2)):
        wide = 256 if p < 4 else 128
        right = cb[lax.rem(block + 2 * p, 16)]
        if p < 4:
            right = jnp.concatenate([right, cb[lax.rem(block + 2 * p + 1, 16)]], axis=0)
        res = mm(mine, right, (((1,), (1,)), ((), ())))
        gf[:, 256 * p:256 * p + wide] = res
        gb[:, 256 * p:256 * p + wide] = res.astype(BF)
        if i is not None:
            cols = pl.ds(384 * i, 384)
            sums.append([go(gb.at[strip(turn(t, k)), cols], gr.at[t, :, cols], at_t(k)) for k in (1, 3, 2)])

    class Turn:
        def __init__(self, axis, colour, done, fixed=None, offset=0):
            self.axis, self.done, self.fixed, self.offset = axis, done, fixed, offset
            self.cols = pl.ds(384 * colour, 384)
            self.to = (at_x, at_y, at_t)[axis]
            self.sent = [go(self.piece(0), self.piece(0), self.to(k)) for k in ((1, -1) if done else (1, -1, 2))]

        def piece(self, k, half=None):
            spots = [x, y, t]
            if self.fixed is not None:
                spots[self.fixed] = turn(spots[self.fixed], self.offset)
            spots[self.axis] = turn(spots[self.axis], k)
            ix, iy, it = spots[0], spots[1], strip(spots[2])
            if half is None:
                whole = {0: pl.ds(0, 4), 1: pl.ds(0, 4), 2: pl.ds(0, 128)}
            else:
                whole = {0: pl.ds(2 * half, 2), 1: pl.ds(2 * half, 2), 2: pl.ds(64 * half, 64)}
            ix = whole[0] if self.done == 0 + 1 else ix
            iy = whole[1] if self.done == 1 + 1 else iy
            it = whole[2] if self.done == 2 + 1 else it
            return gp.at[iy, ix, it, self.cols]

        def take(self):
            self.sent[0].wait_recv()
            self.on_right = go(self.piece(-1, 0), self.piece(-1, 0), self.to(1))
            self.sent[1].wait_recv()
            self.on_left = go(self.piece(1, 1), self.piece(1, 1), self.to(-1))

        def end(self):
            self.on_right.wait_recv()
            self.on_left.wait_recv()

    orders = ((2, 1, 0), (0, 2, 1), (1, 0, 2))

    firsts = []
    for i, order in enumerate(orders):
        cols = pl.ds(384 * i, 384)
        for hop in sums[i]:
            hop.wait_recv()
        total = gf[strip(t), cols]
        for k in (1, 2, 3):
            total = total + gr[turn(t, k), :, cols].astype(F32)
        gp[y, x, strip(t), cols] = total.astype(BF)
        firsts.append(Turn(order[0], i, 0))

    spread = dd[...]
    dev = jnp.sqrt(spread * (1.0 / (rows - 1.0)) + EPS)
    rate = jnp.where(dev < 1.0, 25.0 / ((rows - 1.0) * dev), 0.0) + cov * spread
    dd[...] = rate

    def plain(n, _):
        j, p = lax.div(n, 2), lax.rem(n, 2)
        cols = pl.ds(pl.multiple_of(256 * n, 256), 256)
        at = pl.ds(pl.multiple_of(256 * p, 256), 256)
        right = cb[:, :, cols].reshape(2048, 256)
        acc[j, :, at] = (sign * alpha) * dsum[...] * mu[:, cols] - mm(ht[c], right) * dd[:, cols]
        return 0

    lax.fori_loop(0, 2, plain, 0)
    for first in firsts:
        for copy in first.sent:
            copy.wait_recv()
    seconds = [Turn(b, i, a + 1) for i, (a, b, d) in enumerate(orders)]

    def third(offset):
        return [Turn(d, i, a + 1, b, offset) for i, (a, b, d) in enumerate(orders)]

    def take(turns):
        for one in turns:
            one.take()

    def end(turns):
        for one in turns:
            one.end()

    thirds = {0: third(0)}
    lax.fori_loop(2, 5, plain, 0)
    take(seconds)
    thirds[-1] = third(-1)
    thirds[1] = third(1)
    take(thirds[0])
    end(seconds)
    thirds[2] = third(2)
    lax.fori_loop(5, 8, plain, 0)
    take(thirds[-1])
    take(thirds[1])
    take(thirds[2])
    for offset in (0, -1, 1):
        thirds[offset][0].end()
    for copy in early:
        copy.wait_send()

    def put(by, bx, js):
        b = 4 * by + bx
        here = pl.ds(pl.multiple_of(128 * b, 128), 128)
        for j in js:
            other = lax.rem(b + j, 16)
            tile = gp[by, bx, :, 128 * j:128 * j + 128]
            zb[b, :, pl.ds(pl.multiple_of(128 * other, 128), 128)] = tile
            if 0 < j < 8:
                zb[other, :, here] = tile.T

    def put_early(i, _):
        put(lax.rem(y + 3 + lax.div(i, 4), 4), lax.rem(i, 4), range(3))
        return 0

    lax.fori_loop(0, 12, put_early, 0)
    for offset in (0, -1, 1):
        end(thirds[offset][1:])
    end(thirds[2])

    for copy in started:
        copy.wait_send()
    started.clear()

    def put_last(i, _):
        put(turn(y, 2), i, range(3))
        return 0

    def put_rest(b, _):
        put(lax.div(b, 4), lax.rem(b, 4), range(3, 9))
        return 0

    lax.fori_loop(0, 4, put_last, 0)
    lax.fori_loop(0, 16, put_rest, 0)

    def factor(n, _):
        cols = pl.ds(pl.multiple_of(512 * n, 512), 512)
        res = mm(ht[c], zb[:, :, cols].reshape(2048, 512))
        diff = ht[0, :, cols].astype(F32) - ht[1, :, cols].astype(F32)
        lt[:, cols] = (cov * res + (sign * alpha) * diff).astype(BF)
        return 0

    lax.fori_loop(0, 4, factor, 0)

    theirs = pl.ds(pl.multiple_of(256 * (1 - c), 256), 256)
    ours = pl.ds(pl.multiple_of(256 * c, 256), 256)

    spots = ((0, 0, 512), (1, 0, 512), (2, 0, 512), (3, 0, 256), (3, 256, 256))
    give, stores = [], []

    for n, (j, low, wide) in enumerate(spots):
        at = pl.ds(low, wide)
        where = pl.ds(512 * j + low, wide)
        right = cb[:, :, 512 * j + low:512 * j + low + wide].reshape(2048, wide)
        acc[j, :, at] += mm(lt[...], right)
        give.append(go(acc.at[j, theirs, at], out.at[:, where], partner))
        stores.append(load(acc.at[j, ours, at], kept.at[:, where], 8 + n))
        stores[n].start()
    for copy in give:
        copy.wait_recv()
    for copy in started:
        copy.wait_send()
    for copy in stores:
        copy.wait()


def body(hidden_a, hidden_b, weight):
    anywhere = pl.BlockSpec(memory_space=pl.ANY)
    vm = pltpu.VMEM
    kept, given = pl.pallas_call(
        kernel,
        out_shape=[jax.ShapeDtypeStruct((256, 2048), F32)] * 2,
        in_specs=[anywhere] * 3,
        out_specs=[anywhere] * 2,
        scratch_shapes=[
            vm((2, 512, 1024), BF), vm((1024, 2048), BF), vm((4, 512, 512), F32),
            vm((4, 512, 512), BF), vm((4, 512, 512), BF),
            vm((4, 128, 512), BF), vm((4, 128, 512), BF), vm((4, 128, 512), BF),
            vm((4, 128, 512), BF), vm((4, 128, 512), BF), vm((4, 128, 512), BF),
            vm((16, 128, 2048), BF), vm((16, 128, 2048), BF), vm((2, 2, 4, 512, 256), BF),
            vm((2, 512, 2048), BF), vm((4, 1, 2048), F32), vm((4, 1, 2048), F32),
            vm((1, 2048), F32), vm((1, 2048), F32), vm((512, 1), F32),
            vm((128, 1152), F32), vm((128, 1152), BF), vm((4, 32, 1152), BF),
            vm((4, 4, 128, 1152), BF), vm((512, 2048), BF),
            pltpu.SemaphoreType.DMA((NSEM,)), pltpu.SemaphoreType.DMA((NSEM,)),
            pltpu.SemaphoreType.DMA((16,)),
        ],
        compiler_params=pltpu.CompilerParams(
            collective_id=0, has_side_effects=True, vmem_limit_bytes=VMEM),
        name="vicreg_grad",
    )(hidden_a, hidden_b, weight)
    return kept + given


def solution(mesh):
    placed = (P("crop", "dp"), P("crop", "dp"), P("dp", "tensor"))
    return jax.shard_map(
        body, mesh=mesh, in_specs=placed, out_specs=P(("dp", "crop"), "tensor"), check_vma=False
    )
```
